8 devices in a mesh: data: 1 (over z), dap: 8 (over y, x, core).
Axes of the slice: x: 2, y: 2, z: 1, core: 2. Of those that a mesh axis runs over, the one named last changes fastest.
Arguments:
- pair_act: bfloat16 [768, 768, 128], P(('data', 'dap'))
- pair_mask: int32 [768, 768], P(('data', 'dap'))
- d_pair_out: bfloat16 [768, 768, 128], P(('data', 'dap'))
- ln_pair: bfloat16 [2, 2, 128], replicated
- w_proj: bfloat16 [2, 128, 512], replicated
- w_gate: bfloat16 [2, 128, 128], replicated
- ln_chan: bfloat16 [2, 2, 128], replicated
- w_out: bfloat16 [2, 128, 128], replicated
Outputs:
- output 1: bfloat16 [768, 768, 128], P(('data', 'dap'))
- output 2: bfloat16 [768, 768, 128], P(('data', 'dap'))
- output 3: bfloat16 [2, 2, 128], P('data')
- output 4: bfloat16 [2, 128, 512], P('data')
- output 5: bfloat16 [2, 128, 128], P('data')
- output 6: bfloat16 [2, 2, 128], P('data')
- output 7: bfloat16 [2, 128, 128], P('data')
All inputs are finite; a program needn't handle non-finite values.
Results may differ from the reference program's by a relative error of at most 0.0133311.
Values are sent between devices in bfloat16 or wider.
A program may use at most 1 GiB of HBM per device.

```python
import jax
import jax.numpy as jnp
from jax import lax

N = 768
CZ = 128
CH = 128
LN_EPS = 1e-5


def layer_norm(values, gain_vec, shift_vec, norm_axis):
    mean_val = jnp.mean(values, axis=norm_axis, keepdims=True)
    centered = values - mean_val
    variance = jnp.mean(centered * centered, axis=norm_axis, keepdims=True)
    return centered * lax.rsqrt(variance + LN_EPS) * gain_vec + shift_vec


def draw_mask(mask_key):
    key_row, key_col, key_rhole, key_chole = jax.random.split(mask_key, 4)
    row_keep = jax.random.randint(key_row, (N,), 0, 25) != 0
    col_keep = jax.random.randint(key_col, (N,), 0, 25) != 0
    row_index = jnp.arange(N)
    row_keep = row_keep & (row_index != jax.random.randint(key_rhole, (), 0, N))
    col_keep = col_keep & (row_index != jax.random.randint(key_chole, (), 0, N))
    return (row_keep[:, None] & col_keep[None, :]).astype(jnp.int32)


def setup_inputs(seed: int = 0, part: int = 0) -> dict:
    part_key = jax.random.fold_in(jax.random.key(seed), part)
    key_act, key_grad, key_mask = jax.random.split(part_key, 3)
    shared = jax.random.split(jax.random.key(seed + 1), 7)
    pair_act = jax.random.normal(key_act, (N, N, CZ), jnp.float32).astype(jnp.bfloat16)
    d_pair_out = jax.random.normal(key_grad, (N, N, CZ), jnp.float32).astype(jnp.bfloat16)
    pair_mask = draw_mask(key_mask)
    ln_pair = jnp.stack([1.0 + 0.3 * jax.random.normal(shared[0], (2, CZ), jnp.float32), 0.3 * jax.random.normal(shared[1], (2, CZ), jnp.float32)], axis=1).astype(jnp.bfloat16)
    w_proj = (jax.random.normal(shared[2], (2, CZ, 4 * CH), jnp.float32) * CZ ** -0.5).astype(jnp.bfloat16)
    w_gate = (jax.random.normal(shared[3], (2, CZ, CZ), jnp.float32) * CZ ** -0.5).astype(jnp.bfloat16)
    ln_chan = jnp.stack([1.0 + 0.3 * jax.random.normal(shared[4], (2, CH), jnp.float32), 0.3 * jax.random.normal(shared[5], (2, CH), jnp.float32)], axis=1).astype(jnp.bfloat16)
    w_out = (jax.random.normal(shared[6], (2, CH, CZ), jnp.float32) * CH ** -0.5).astype(jnp.bfloat16)
    return {'pair_act': pair_act, 'pair_mask': pair_mask, 'd_pair_out': d_pair_out, 'ln_pair': ln_pair, 'w_proj': w_proj, 'w_gate': w_gate, 'ln_chan': ln_chan, 'w_out': w_out}


def project_rows(z_rows, mask_rows, ln_p, w_proj, w_gate):
    x_norm = layer_norm(z_rows, ln_p[0], ln_p[1], -1).astype(jnp.bfloat16).astype(jnp.float32)
    proj_all = jnp.einsum('ijd,de->eij', x_norm, w_proj)
    gate_val = jax.nn.sigmoid(jnp.einsum('ijd,de->ije', x_norm, w_gate))
    lin_a, pre_ga, lin_b, pre_gb = jnp.split(proj_all, 4, axis=0)
    mask_f = mask_rows.astype(jnp.float32)
    left_proj = (mask_f * jax.nn.sigmoid(pre_ga) * lin_a).astype(jnp.bfloat16)
    right_proj = (mask_f * jax.nn.sigmoid(pre_gb) * lin_b).astype(jnp.bfloat16)
    return left_proj, right_proj, gate_val


def tri_outgoing(left_grp, right_grp):
    return jnp.einsum('cik,cjk->cij', left_grp.astype(jnp.float32), right_grp.astype(jnp.float32)).astype(jnp.bfloat16)


def tri_incoming(left_grp, right_grp):
    return jnp.einsum('cki,ckj->cij', left_grp.astype(jnp.float32), right_grp.astype(jnp.float32)).astype(jnp.bfloat16)


def finish_rows(z_rows, t_rows, gate_val, ln_q, w_out):
    y_norm = layer_norm(t_rows.astype(jnp.float32), ln_q[0][:, None, None], ln_q[1][:, None, None], 0).astype(jnp.bfloat16).astype(jnp.float32)
    update_f = jnp.einsum('cij,cd->ijd', y_norm, w_out)
    return (z_rows + gate_val * update_f).astype(jnp.bfloat16)


def tri_update(z_pair, pair_mask, ln_p, w_proj, w_gate, ln_q, w_out, incoming):
    z_blocks = z_pair.astype(jnp.float32).reshape(N // 8, 8, N, CZ)
    mask_blocks = pair_mask.reshape(N // 8, 8, N)
    prep_fn = jax.checkpoint(project_rows)
    left_blk, right_blk, gate_blk = lax.map(lambda block_in: prep_fn(block_in[0], block_in[1], ln_p, w_proj, w_gate), (z_blocks, mask_blocks))
    left_groups = jnp.swapaxes(left_blk, 0, 1).reshape(8, CH // 8, N, N)
    right_groups = jnp.swapaxes(right_blk, 0, 1).reshape(8, CH // 8, N, N)
    tri_fn = jax.checkpoint(tri_incoming if incoming else tri_outgoing)
    t_groups = lax.map(lambda block_in: tri_fn(block_in[0], block_in[1]), (left_groups, right_groups))
    t_blocks = jnp.swapaxes(t_groups.reshape(CH, N // 8, 8, N), 0, 1)
    post_fn = jax.checkpoint(finish_rows)
    out_blocks = lax.map(lambda block_in: post_fn(block_in[0], block_in[1], block_in[2], ln_q, w_out), (z_blocks, t_blocks, gate_blk))
    return out_blocks.reshape(N, N, CZ)


def reference(pair_act, pair_mask, d_pair_out, ln_pair, w_proj, w_gate, ln_chan, w_out):
    def forward(z_in, ln_pair_in, w_proj_in, w_gate_in, ln_chan_in, w_out_in):
        ln_pf = ln_pair_in.astype(jnp.float32)
        proj_f = w_proj_in.astype(jnp.float32)
        gate_f = w_gate_in.astype(jnp.float32)
        ln_qf = ln_chan_in.astype(jnp.float32)
        out_f = w_out_in.astype(jnp.float32)
        z_mid = tri_update(z_in, pair_mask, ln_pf[0], proj_f[0], gate_f[0], ln_qf[0], out_f[0], False)
        return tri_update(z_mid, pair_mask, ln_pf[1], proj_f[1], gate_f[1], ln_qf[1], out_f[1], True)
    pair_out, pull_back = jax.vjp(forward, pair_act, ln_pair, w_proj, w_gate, ln_chan, w_out)
    d_pair, d_ln_p, d_w_p, d_w_g, d_ln_q, d_w_o = pull_back(d_pair_out)
    return pair_out, d_pair, d_ln_p, d_w_p, d_w_g, d_ln_q, d_w_o
```

```python
import functools

import jax
import jax.numpy as jnp
from jax import lax
from jax.experimental import pallas as pl
from jax.experimental.pallas import tpu as pltpu
from jax.sharding import PartitionSpec as P

LN_EPS = 1e-5
AXIS = 'dap'
NDEV = 8
N = 768
C = 128
G = C // NDEV
ROWS = N // NDEV
R = 3
RC = ROWS // R
M = NDEV * RC
LB = 256
RB = 4
BF = jnp.bfloat16
F32 = jnp.float32


def dotg(lhs, rhs, lc, rc):
    return lax.dot_general(lhs, rhs, (((lc,), (rc,)), ((), ())), preferred_element_type=F32)


def norm_z(z_val, ln_p):
    zf = z_val.astype(F32)
    centered = zf - jnp.mean(zf, axis=1, keepdims=True)
    rstd = lax.rsqrt(jnp.mean(centered * centered, axis=1, keepdims=True) + LN_EPS)
    hat = centered * rstd
    return (hat * ln_p[0:1] + ln_p[1:2]).astype(BF), hat, rstd


def norm_t(t_val, gain, shift):
    tf = t_val.astype(F32)
    centered = tf - jnp.mean(tf, axis=0, keepdims=True)
    rstd = lax.rsqrt(jnp.mean(centered * centered, axis=0, keepdims=True) + LN_EPS)
    hat = centered * rstd
    return (hat * gain + shift).astype(BF), hat, rstd


def project(x_val, wp_t):
    proj = dotg(wp_t, x_val, 1, 1)
    return proj[0:C], jax.nn.sigmoid(proj[C:2 * C]), proj[2 * C:3 * C], jax.nn.sigmoid(proj[3 * C:4 * C])


def store_ab(ab_ref, row, cols, x_val, wp_t, mask):
    lin_a, sig_a, lin_b, sig_b = project(x_val, wp_t)
    ab_ref[:, 0, row, :, cols] = (mask * sig_a * lin_a).astype(BF).reshape(NDEV, G, LB)
    ab_ref[:, 1, row, :, cols] = (mask * sig_b * lin_b).astype(BF).reshape(NDEV, G, LB)


def gate_update(x_val, y_val, w_gate, w_out):
    return jax.nn.sigmoid(dotg(x_val, w_gate, 1, 0)), dotg(y_val, w_out, 0, 0)


def lane_fold(val):
    return val[:, 0:128] + val[:, 128:256]


def row_fold(val):
    return jnp.sum(val.reshape(LB // 8, 8, C), axis=0)


def finish_back(d_f, gate, upd, x_val, y_val, t_hat, t_rstd, gain, w_out, dt_ref, dg_ref, row, cols, acc):
    gwo_ref, gwg_ref, glq_ref = acc
    d_gate = (d_f * upd * gate * (1.0 - gate)).astype(BF)
    d_upd = (d_f * gate).astype(BF)
    dg_ref[row, cols, :] = d_gate
    gwo_ref[...] += dotg(y_val, d_upd, 1, 0)
    gwg_ref[...] += dotg(x_val, d_gate, 0, 0)
    d_y = dotg(w_out, d_upd, 1, 1).astype(BF).astype(F32)
    glq_ref[0] += lane_fold(d_y * t_hat)
    glq_ref[1] += lane_fold(d_y)
    d_hat = d_y * gain
    m_one = jnp.mean(d_hat, axis=0, keepdims=True)
    m_two = jnp.mean(d_hat * t_hat, axis=0, keepdims=True)
    d_t = t_rstd * (d_hat - m_one - t_hat * m_two)
    dt_ref[:, row, :, cols] = d_t.astype(BF).reshape(NDEV, G, LB)


def project_back(x_val, hat, rstd, ln_p, wp_t, w_gate, mask, d_a, d_b, d_gate, d_f, acc):
    gwp_ref, glp_ref = acc
    lin_a, sig_a, lin_b, sig_b = project(x_val, wp_t)
    d_a = d_a.astype(F32) * mask
    d_b = d_b.astype(F32) * mask
    da_s = d_a * sig_a
    db_s = d_b * sig_b
    d_proj = jnp.concatenate([da_s.astype(BF), (da_s * lin_a * (1.0 - sig_a)).astype(BF), db_s.astype(BF), (db_s * lin_b * (1.0 - sig_b)).astype(BF)], axis=0)
    gwp_ref[...] += dotg(d_proj, x_val, 1, 0)
    d_x = (dotg(d_proj, wp_t, 0, 0) + dotg(d_gate, w_gate, 1, 1)).astype(BF).astype(F32)
    glp_ref[0] += row_fold(d_x * hat)
    glp_ref[1] += row_fold(d_x)
    d_hat = d_x * ln_p[0:1]
    m_one = jnp.mean(d_hat, axis=1, keepdims=True)
    m_two = jnp.mean(d_hat * hat, axis=1, keepdims=True)
    return (d_f + rstd * (d_hat - m_one - hat * m_two)).astype(BF)


def each_block(body):
    @pl.loop(0, RB)
    def _(row):
        for q in range(N // LB):
            body(row, slice(q * LB, (q + 1) * LB))


def zero_first(refs):
    @pl.when(pl.program_id(0) == 0)
    def _():
        for ref in refs:
            ref[...] = jnp.zeros_like(ref)


def load_mask(m_ref, row, cols):
    return m_ref[row, :, cols].astype(F32)


def load_t(t_ref, row, cols):
    return t_ref[:, row, :, cols].reshape(C, LB)


def body_a(z_ref, m_ref, lnp_ref, wp_ref, ab_ref):
    def one(row, cols):
        x_val, _, _ = norm_z(z_ref[row, cols, :], lnp_ref[...])
        store_ab(ab_ref, row, cols, x_val, wp_ref[...], load_mask(m_ref, row, cols))
    each_block(one)


def body_b(z_ref, t_ref, m_ref, lnp_ref, wg_ref, lnq_ref, wo_ref, lnp2_ref, wp2_ref, zn_ref, ab_ref):
    def one(row, cols):
        z_val = z_ref[row, cols, :]
        x_val, _, _ = norm_z(z_val, lnp_ref[...])
        y_val, _, _ = norm_t(load_t(t_ref, row, cols), lnq_ref[0], lnq_ref[1])
        gate, upd = gate_update(x_val, y_val, wg_ref[...], wo_ref[...])
        z_new = (z_val.astype(F32) + gate * upd).astype(BF)
        zn_ref[row, cols, :] = z_new
        x_new, _, _ = norm_z(z_new, lnp2_ref[...])
        store_ab(ab_ref, row, cols, x_new, wp2_ref[...], load_mask(m_ref, row, cols))
    each_block(one)


def body_c(z_ref, t_ref, g_ref, lnp_ref, wg_ref, lnq_ref, wo_ref, *rest):
    zn_ref, dt_ref, dg_ref, gwo_ref, gwg_ref, glq_ref = rest[-6:]
    zero_first((gwo_ref, gwg_ref, glq_ref))

    def one(row, cols):
        z_val = z_ref[row, cols, :]
        x_val, _, _ = norm_z(z_val, lnp_ref[...])
        y_val, t_hat, t_rstd = norm_t(load_t(t_ref, row, cols), lnq_ref[0], lnq_ref[1])
        gate, upd = gate_update(x_val, y_val, wg_ref[...], wo_ref[...])
        zn_ref[row, cols, :] = (z_val.astype(F32) + gate * upd).astype(BF)
        d_f = g_ref[row, cols, :].astype(F32)
        finish_back(d_f, gate, upd, x_val, y_val, t_hat, t_rstd, lnq_ref[0], wo_ref[...], dt_ref, dg_ref, row, cols, (gwo_ref, gwg_ref, glq_ref))
    each_block(one)


def body_d(zm_ref, dab_ref, dgm_ref, g_ref, m_ref, lnp2_ref, wp2_ref, wg2_ref, z_ref, t_ref, lnp_ref, wg_ref, lnq_ref, wo_ref,
           dm_ref, dt_ref, dg_ref, gwp_ref, glp_ref, gwo_ref, gwg_ref, glq_ref):
    zero_first((gwp_ref, glp_ref, gwo_ref, gwg_ref, glq_ref))

    def one(row, cols):
        x2, hat2, rstd2 = norm_z(zm_ref[row, cols, :], lnp2_ref[...])
        d_mid = project_back(x2, hat2, rstd2, lnp2_ref[...], wp2_ref[...], wg2_ref[...], load_mask(m_ref, row, cols),
                             dab_ref[:, 0, row, :, cols].reshape(C, LB), dab_ref[:, 1, row, :, cols].reshape(C, LB),
                             dgm_ref[row, cols, :], g_ref[row, cols, :].astype(F32), (gwp_ref, glp_ref))
        dm_ref[row, cols, :] = d_mid
        x_val, _, _ = norm_z(z_ref[row, cols, :], lnp_ref[...])
        y_val, t_hat, t_rstd = norm_t(load_t(t_ref, row, cols), lnq_ref[0], lnq_ref[1])
        gate, upd = gate_update(x_val, y_val, wg_ref[...], wo_ref[...])
        finish_back(d_mid.astype(F32), gate, upd, x_val, y_val, t_hat, t_rstd, lnq_ref[0], wo_ref[...], dt_ref, dg_ref, row, cols, (gwo_ref, gwg_ref, glq_ref))
    each_block(one)


def body_e(z_ref, da_ref, db_ref, dg_ref, dm_ref, m_ref, lnp_ref, wp_ref, wg_ref, *rest):
    dz_ref, gwp_ref, glp_ref = rest[-3:]
    zero_first((gwp_ref, glp_ref))

    def one(row, cols):
        x_val, hat, rstd = norm_z(z_ref[row, cols, :], lnp_ref[...])
        dz_ref[row, cols, :] = project_back(x_val, hat, rstd, lnp_ref[...], wp_ref[...], wg_ref[...], load_mask(m_ref, row, cols),
                                            load_t(da_ref, row, cols), load_t(db_ref, row, cols),
                                            dg_ref[row, cols, :], dm_ref[row, cols, :].astype(F32), (gwp_ref, glp_ref))
    each_block(one)


STEPS = RC // RB


def full_rows(chunk):
    return pl.BlockSpec((RB, N, C), lambda i: (chunk * STEPS + i, 0, 0))


def mask_rows(chunk):
    return pl.BlockSpec((RB, 1, N), lambda i: (chunk * STEPS + i, 0, 0))


PIECE = pl.BlockSpec((RB, N, C), lambda i: (i, 0, 0))
CHAN = pl.BlockSpec((NDEV, RB, G, N), lambda i: (0, i, 0, 0))
CHAN2 = pl.BlockSpec((NDEV, 2, RB, G, N), lambda i: (0, 0, i, 0, 0))
CHAN_T = jax.ShapeDtypeStruct((NDEV, RC, G, N), BF)
CHAN2_T = jax.ShapeDtypeStruct((NDEV, 2, RC, G, N), BF)
PIECE_T = jax.ShapeDtypeStruct((RC, N, C), BF)
FULL_T = jax.ShapeDtypeStruct((ROWS, N, C), BF)


def whole(shape):
    return pl.BlockSpec(shape, lambda i: (0,) * len(shape))


def acc(shape):
    return whole(shape), jax.ShapeDtypeStruct(shape, F32)


GWP = acc((4 * C, C))
GLP = acc((2, 8, C))
GWO = acc((C, C))
GWG = acc((C, C))
GLQ = acc((2, C, 128))
ANY = pl.BlockSpec(memory_space=pl.ANY)


def call(body, name, grid, in_specs, outs, flops, args, aliases=None, scratch=()):
    return pl.pallas_call(
        body,
        grid=(grid,),
        in_specs=in_specs,
        out_specs=[spec for spec, _ in outs],
        out_shape=[shape for _, shape in outs],
        scratch_shapes=list(scratch),
        input_output_aliases=aliases or {},
        compiler_params=pltpu.CompilerParams(dimension_semantics=('arbitrary',), vmem_limit_bytes=58 * 1024 * 1024),
        cost_estimate=pl.CostEstimate(flops=flops, bytes_accessed=60_000_000, transcendentals=0),
        name=name,
    )(*args)


POS = RC * N
UNIT = 2 * POS * C * C


def place(dst, parts):
    for chunk, part in enumerate(parts):
        for dev in range(NDEV):
            dst[dev * ROWS + chunk * RC:dev * ROWS + (chunk + 1) * RC, :] = part[dev * RC:(dev + 1) * RC, :]


def split_rows(full, outs):
    for chunk, out in enumerate(outs):
        for dev in range(NDEV):
            out[dev * RC:(dev + 1) * RC, :] = full[dev * ROWS + chunk * RC:dev * ROWS + (chunk + 1) * RC, :]


def tri_rows(lhs, b0, b1, b2, out, full, *, rhs_dim):
    place(full, (b0, b1, b2))
    out[...] = dotg(lhs[...], full[...], 1, rhs_dim).astype(BF)


def tri_sum(a0, a1, a2, b0, b1, b2, o0, o1, o2):
    total = dotg(a0[...], b0[...], 0, 0) + dotg(a1[...], b1[...], 0, 0) + dotg(a2[...], b2[...], 0, 0)
    split_rows(total.astype(BF), (o0, o1, o2))


def tri_pair(a_r, b_r, d0, d1, d2, out, full):
    place(full, (d0, d1, d2))
    out[0] = dotg(b_r[...], full[...], 1, 1).astype(BF)
    out[1] = dotg(a_r[...], full[...], 1, 0).astype(BF)


SQ = None


def chan(which=None):
    if which is None:
        return pl.BlockSpec((None, M, N), lambda c: (c, 0, 0))
    return pl.BlockSpec((None, None, M, N), lambda c: (which, c, 0, 0))


TRI_T = jax.ShapeDtypeStruct((G, M, N), BF)
TRI = (pl.BlockSpec((None, M, N), lambda c: (c, 0, 0)), TRI_T)
TRI2 = (pl.BlockSpec((2, None, M, N), lambda c: (0, c, 0, 0)), jax.ShapeDtypeStruct((2, G, M, N), BF))
FULL = (pltpu.VMEM((N, N), BF),)
TRI_FLOPS = 2 * G * M * N * N


def arrive2(x):
    return jnp.transpose(x, (1, 3, 0, 2, 4)).reshape(2, G, M, N)


def arrive(x):
    return jnp.transpose(x, (2, 0, 1, 3)).reshape(G, M, N)


def leave(x):
    return jnp.transpose(x.reshape(G, NDEV, RC, N), (1, 2, 0, 3))


def leave2(x):
    return jnp.transpose(x.reshape(2, G, NDEV, RC, N), (2, 0, 3, 1, 4))


def exchange(x, name):
    with jax.named_scope(name):
        return lax.all_to_all(x, AXIS, 0, 0)


def device_step(pair_act, pair_mask, d_pair_out, ln_pair, w_proj, w_gate, ln_chan, w_out):
    mask = pair_mask.reshape(ROWS, 1, N)
    lnp = [ln_pair[u].astype(F32) for u in range(2)]
    wpt = [w_proj[u].T for u in range(2)]
    lnq = [jnp.broadcast_to(ln_chan[u].astype(F32)[:, :, None], (2, C, LB)) for u in range(2)]
    S_LNP, S_WP, S_W, S_LNQ = whole((2, C)), whole((4 * C, C)), whole((C, C)), whole((2, C, LB))
    rng = range(R)

    ab = [call(body_a, f'pos_a{r}', STEPS, [full_rows(r), mask_rows(r), S_LNP, S_WP], [(CHAN2, CHAN2_T)], 4 * UNIT,
               (pair_act, mask, lnp[0], wpt[0]))[0] for r in rng]
    ab = [arrive2(exchange(ab[r], f'x_ab{r}')) for r in rng]
    t_out = []
    for r in rng:
        t_r = call(functools.partial(tri_rows, rhs_dim=1), f'tri_of{r}', G, [chan(0)] + [chan(1)] * 3, [TRI], TRI_FLOPS,
                   (ab[r], ab[0], ab[1], ab[2]), scratch=FULL)[0]
        t_out.append(exchange(leave(t_r), f'x_t{r}'))

    z_mid, ab2 = [], []
    for r in rng:
        z_r, ab_r = call(body_b, f'pos_b{r}', STEPS,
                         [full_rows(r), CHAN, mask_rows(r), S_LNP, S_W, S_LNQ, S_W, S_LNP, S_WP],
                         [(PIECE, PIECE_T), (CHAN2, CHAN2_T)], 6 * UNIT,
                         (pair_act, t_out[r], mask, lnp[0], w_gate[0], lnq[0], w_out[0], lnp[1], wpt[1]))
        z_mid.append(z_r)
        ab2.append(arrive2(exchange(ab_r, f'x_ab2{r}')))
    t_in = call(tri_sum, 'tri_if', G, [chan(0)] * 3 + [chan(1)] * 3, [TRI] * 3, 3 * TRI_FLOPS, tuple(ab2) * 2)
    t_in = [exchange(leave(t_in[r]), f'x_t2{r}') for r in rng]

    pair_out = None
    d_t2, d_gate2, acc_c = [], [], []
    for r in rng:
        ins = [PIECE, CHAN, full_rows(r), S_LNP, S_W, S_LNQ, S_W]
        args = (z_mid[r], t_in[r], d_pair_out, lnp[1], w_gate[1], lnq[1], w_out[1])
        aliases = {}
        if pair_out is not None:
            aliases = {len(ins): 0}
            ins, args = ins + [ANY], args + (pair_out,)
        pair_out, dt_r, dg_r, *grads = call(body_c, f'pos_c{r}', STEPS, ins,
                                            [(full_rows(r), FULL_T), (CHAN, CHAN_T), (PIECE, PIECE_T), GWO, GWG, GLQ], 6 * UNIT,
                                            args, aliases)
        d_t2.append(arrive(exchange(dt_r, f'x_dt2{r}')))
        d_gate2.append(dg_r)
        acc_c.append(grads)

    d_mid, d_t, d_gate, acc_d = [], [], [], []
    for r in rng:
        dab = call(tri_pair, f'tri_ib{r}', G, [chan(0), chan(1)] + [chan()] * 3, [TRI2], 2 * TRI_FLOPS,
                   (ab2[r], ab2[r], d_t2[0], d_t2[1], d_t2[2]), scratch=FULL)[0]
        dab = exchange(leave2(dab), f'x_dab2{r}')
        dm_r, dt_r, dg_r, *grads = call(
            body_d, f'pos_d{r}', STEPS,
            [PIECE, CHAN2, PIECE, full_rows(r), mask_rows(r), S_LNP, S_WP, S_W, full_rows(r), CHAN, S_LNP, S_W, S_LNQ, S_W],
            [(PIECE, PIECE_T), (CHAN, CHAN_T), (PIECE, PIECE_T), GWP, GLP, GWO, GWG, GLQ], 18 * UNIT,
            (z_mid[r], dab, d_gate2[r], d_pair_out, mask, lnp[1], wpt[1], w_gate[1],
             pair_act, t_out[r], lnp[0], w_gate[0], lnq[0], w_out[0]))
        d_mid.append(dm_r)
        d_t.append(arrive(exchange(dt_r, f'x_dt{r}')))
        d_gate.append(dg_r)
        acc_d.append(grads)

    d_b = call(tri_sum, 'tri_ob', G, [chan()] * 3 + [chan(0)] * 3, [TRI] * 3, 3 * TRI_FLOPS, tuple(d_t) + tuple(ab))
    d_pair = None
    acc_e = []
    for r in rng:
        da_r = call(functools.partial(tri_rows, rhs_dim=0), f'tri_oa{r}', G, [chan()] + [chan(1)] * 3, [TRI], TRI_FLOPS,
                    (d_t[r], ab[0], ab[1], ab[2]), scratch=FULL)[0]
        da_r = exchange(leave(da_r), f'x_da{r}')
        db_r = exchange(leave(d_b[r]), f'x_db{r}')
        ins = [full_rows(r), CHAN, CHAN, PIECE, PIECE, mask_rows(r), S_LNP, S_WP, S_W]
        args = (pair_act, da_r, db_r, d_gate[r], d_mid[r], mask, lnp[0], wpt[0], w_gate[0])
        aliases = {}
        if d_pair is not None:
            aliases = {len(ins): 0}
            ins, args = ins + [ANY], args + (d_pair,)
        d_pair, *grads = call(body_e, f'pos_e{r}', STEPS, ins, [(full_rows(r), FULL_T), GWP, GLP], 13 * UNIT, args, aliases)
        acc_e.append(grads)

    total = lambda parts: [sum(vals[1:], vals[0]) for vals in zip(*parts)]
    gwo1, gwg1, glq1 = total(acc_c)
    gwp1, glp1, gwo0, gwg0, glq0 = total(acc_d)
    gwp0, glp0 = total(acc_e)
    local = (jnp.stack([glp0.sum(1), glp1.sum(1)]), jnp.stack([gwp0.T, gwp1.T]), jnp.stack([gwg0, gwg1]),
             jnp.stack([glq0.sum(2), glq1.sum(2)]), jnp.stack([gwo0, gwo1]))
    grads = lax.psum(local, AXIS)
    return (pair_out, d_pair) + tuple(val.astype(BF) for val in grads)


def solution(mesh):
    row_spec = P(('data', 'dap'), None, None)
    mask_spec = P(('data', 'dap'), None)
    full_spec = P()
    grad_spec = P('data', None, None)
    return jax.shard_map(device_step, mesh=mesh, in_specs=(row_spec, mask_spec, row_spec, full_spec, full_spec, full_spec, full_spec, full_spec), out_specs=(row_spec, row_spec, grad_spec, grad_spec, grad_spec, grad_spec, grad_spec), check_vma=False)
```
